512 devices in a mesh: row: 64 (over z, y), col: 8 (over x, core).
Axes of the slice: x: 4, y: 8, z: 8, core: 2. Of those that a mesh axis runs over, the one named last changes fastest.
Arguments:
- left_site: bfloat16 [1536, 3, 4096], P('row'), may hold values from -6 to 6
- right_site: bfloat16 [4096, 3, 4096], P('row', None, 'col'), may hold values from -0.09375 to 0.09375
- gate: float32 [9, 9], replicated, may hold values from -2 to 2
- probes_matrix: bfloat16 [12288, 256], P('col'), may hold values from -0.0546875 to 0.0546875
Outputs:
- basis: float32 [4608, 256], P('row')
- new_block: float32 [256, 12288], P('row', 'col')
The draws below stay inside these ranges and needn't reach their ends.
All inputs are finite; a program needn't handle non-finite values.
Results may differ from the reference program's by a relative error of at most 0.0044.
Values may be sent and summed in bfloat16 or wider, within the bound.
No kernel may reach another device: no remote copies, remote signals or barrier semaphores. Data moves between devices by JAX's collectives and lax.ppermute only.
A program may use at most 128 MiB of HBM per device.

```python
import jax
import jax.numpy as jnp
from jax import lax

CHI = 4096
CUTOFF = 3
A_DEV = 24
PROBES = 256
LEFT = 1536
ORDER = 12288


def block_levels(own_key, dims, split, smallest, top_value):
    level = 1.0
    for axis_at, blocks in split:
        draws = jax.random.uniform(jax.random.fold_in(jax.random.fold_in(own_key, 6), axis_at), (blocks,), jnp.float32, smallest / len(split), top_value / len(split))
        level = level * jnp.repeat(jnp.exp(draws), dims[axis_at] // blocks).reshape((-1,) + (1,) * (len(dims) - 1 - axis_at))
    return level


def scatter_about(own_key, extent, deviation, most, split=(), kind=jnp.bfloat16):
    array = deviation * jax.random.normal(own_key, extent, jnp.float32)
    if split:
        array = array * block_levels(own_key, extent, split, -0.22, 0.18)
    return jnp.clip(array, -most, most).astype(kind)


def setup_inputs(seed: int = 0) -> dict:
    arg_keys = jax.random.split(jax.random.key(seed), 5)
    left_site = scatter_about(arg_keys[0], (LEFT, CUTOFF, CHI), 1.0, 6.0, ((0, 64),))
    right_site = scatter_about(arg_keys[1], (CHI, CUTOFF, CHI), CHI ** -0.5, 0.09375, ((0, 64), (2, 8)))
    gate = scatter_about(arg_keys[2], (CUTOFF * CUTOFF, CUTOFF * CUTOFF), (CUTOFF * CUTOFF) ** -0.5, 2.0, (), jnp.float32)
    probes_matrix = scatter_about(arg_keys[3], (ORDER, PROBES), ORDER ** -0.5, 0.0546875, ((0, 8),))
    return {"left_site": left_site, "right_site": right_site, "gate": gate, "probes_matrix": probes_matrix}


def reference(left_site, right_site, gate, probes_matrix):
    block_a = 4 * A_DEV
    right_cols = right_site.astype(jnp.float32).reshape(CHI, CUTOFF * CHI)
    gate_four = gate.reshape(CUTOFF, CUTOFF, CUTOFF, CUTOFF)
    left_blocks = left_site.astype(jnp.float32).reshape(LEFT // block_a, block_a * CUTOFF, CHI)
    probes_wide = probes_matrix.astype(jnp.float32)

    def step(carry, left_block):
        gram, projected = carry
        mixed = jnp.dot(left_block, right_cols)
        mixed = mixed.reshape(block_a, CUTOFF, CUTOFF, CHI)
        theta = jnp.einsum('stuv,auvb->asbt', gate_four, mixed, precision=lax.Precision.HIGHEST)
        theta = theta.reshape(block_a * CUTOFF, CHI * CUTOFF).astype(jnp.bfloat16)
        theta_wide = theta.astype(jnp.float32)
        sketch = jnp.dot(theta_wide, probes_wide).astype(jnp.bfloat16)
        sketch_wide = sketch.astype(jnp.float32)
        gram = gram + jnp.dot(sketch_wide.T, sketch_wide, precision=lax.Precision.HIGHEST)
        projected = projected + jnp.dot(sketch_wide.T, theta_wide, precision=lax.Precision.HIGHEST)
        return ((gram, projected), sketch)
    start = (jnp.zeros((PROBES, PROBES), jnp.float32), jnp.zeros((PROBES, CUTOFF * CHI), jnp.float32))
    (gram, projected), sketches = lax.scan(step, start, left_blocks)
    sketch_all = sketches.reshape(CUTOFF * LEFT, PROBES).astype(jnp.float32)
    factor = jnp.linalg.cholesky(gram)
    basis = lax.linalg.triangular_solve(factor, sketch_all, left_side=False, lower=True, transpose_a=True)
    new_block = lax.linalg.triangular_solve(factor, projected, left_side=True, lower=True)
    return (basis, new_block)
```

```python
import jax
import jax.numpy as jnp
from jax import lax
from jax.experimental import pallas as pl
from jax.experimental.pallas import tpu as pltpu
from jax.sharding import PartitionSpec as P


F32 = jnp.float32
BF16 = jnp.bfloat16
HIGHEST = lax.Precision.HIGHEST
ROWS = 64
COLS = 8


def iota(shape, axis):
    return lax.broadcasted_iota(jnp.int32, shape, axis)


def dot(a, b, dims=((1,), (0,)), precision=None):
    return lax.dot_general(a, b, (dims, ((), ())), precision=precision, preferred_element_type=F32)


def stride_three(t, transposed):
    shape = (384, 128) if transposed else (128, 384)
    b, column = iota(shape, int(transposed)), iota(shape, int(not transposed))
    return jnp.where(column == 3 * b + t, 1.0, 0.0).astype(BF16)


def left_kernel(place, left, left_out, lines):
    row, column, lane = iota((16, 72), 0), iota((16, 72), 1), iota((16, 128), 1)
    sides = []
    for h in range(2):
        line = 2 * row + h
        photon = jnp.where(line < 6, 0, jnp.where(line < 12, 1, 2))
        chosen = (column == photon * 24 + 6 * (place[1] // 2) + line - 6 * photon) & (line < 18)
        sides.append(dot(jnp.where(chosen, 1.0, 0.0).astype(BF16), left[...].reshape(72, 4096)))
    for pair in range(ROWS // 2):
        even, odd = (side[:, 128 * pair : 128 * pair + 128] for side in sides)
        first = jnp.where(lane < 64, even, pltpu.roll(odd, 64, 1))
        second = jnp.where(lane < 64, pltpu.roll(even, 64, 1), odd)
        lines[20 * pair : 20 * pair + 10, :] = first[:10]
        lines[20 * pair + 10 : 20 * pair + 20, :] = second[:10]
    left_out[...] = lines[...].astype(BF16)


def first_kernel(gate, right, probes, weight_out, product):
    wide = right[...].reshape(192, 512)
    for t in range(3):
        pick = stride_three(t, False)
        own = jnp.concatenate(
            [dot(pick, probes[384 * j : 384 * j + 384, :]).astype(BF16) for j in range(4)], axis=0
        )
        product[t] = dot(wide, own)
    for up in range(3):
        for s in range(3):
            total = jnp.zeros((64, 256), F32)
            for tp in range(3):
                for t in range(3):
                    total = total + gate[3 * s + t, 3 * up + tp] * product[t, 64 * tp : 64 * tp + 64, :]
            for core in range(2):
                half = total[:, 128 * core : 128 * core + 128]
                weight_out[core, 64 * up : 64 * up + 64, 128 * s : 128 * s + 128] = half


def weight_kernel(pieces, out):
    total = (pieces[0] + pieces[1]).astype(BF16)
    for x in range(4):
        out[x] = total


def sketch_kernel(left_in, weight, sketch_out, left_rows, wide_left, high, low, wide_sketch):
    wide_left[...] = left_in[...].astype(F32)
    side = iota((64, 128), 1) // 64
    for up in range(3):
        for i in range(6):
            line = 6 * up + i
            tile = jnp.where(side == line % 2, wide_left[pl.ds(line // 2, 64, stride=10), :], 0.0)
            left_rows[64 * i : 64 * i + 64, 128 * up : 128 * up + 128] = tile.astype(BF16)
    total = (weight[0].astype(F32) + weight[1].astype(F32)) + (weight[2].astype(F32) + weight[3].astype(F32))
    for part, wide in zip(split(total), (high, low)):
        for up in range(3):
            block = part[64 * up : 64 * up + 64]
            wide[128 * up : 128 * up + 64, :] = block
            wide[128 * up + 64 : 128 * up + 128, :] = block
    for i in range(6):
        rows = left_rows[64 * i : 64 * i + 64, :]
        part = dot(rows, high[...]) + dot(rows, low[...])
        for s in range(3):
            wide_sketch[pl.ds(3 * i + s, 64, stride=18), :] = part[:, 128 * s : 128 * s + 128]
    sketch_out[...] = wide_sketch[...].astype(BF16)


def total_kernel(pieces, own, out, four, many):
    total = pieces[:144, :].astype(F32)
    for k in range(1, 8):
        total = total + pieces[144 * k : 144 * k + 144, :].astype(F32)
    four[...] = total[:72] + total[72:]
    total = four[0:18, :] + four[18:36, :] + four[36:54, :] + four[54:72, :]
    own[:18, :] = total.astype(BF16)
    own[18:, :] = jnp.zeros((6, 128), BF16)
    for k in range(8):
        many[18 * k : 18 * k + 18, :] = total
    total = many[...].astype(BF16)
    for k in range(8):
        out[144 * k : 144 * k + 144, :] = total


def projection_kernel(place, gate, sketch_in, other_in, left_rows, own, out, wide_sketch, sketch, product, cross):
    core = place[1] % 2
    wide_sketch[...] = sketch_in[...].astype(F32)
    for i in range(6):
        for s in range(3):
            tile = wide_sketch[pl.ds(3 * i + s, 64, stride=18), :]
            sketch[64 * i : 64 * i + 64, 128 * s : 128 * s + 128] = tile.astype(BF16)
    for up in range(3):
        part = dot(left_rows[:, 128 * up : 128 * up + 128], sketch[...], ((0,), (0,)))
        product[64 * up : 64 * up + 64, :] = part[:64] + part[64:]
    for tp in range(3):
        for t in range(3):
            total = jnp.zeros((64, 128), F32)
            for up in range(3):
                for s in range(3):
                    part = product[64 * up : 64 * up + 64, 128 * s : 128 * s + 128]
                    total = total + gate[3 * s + t, 3 * up + tp] * part
            line = 64 * (3 * tp + t)
            total = total.astype(BF16)
            for x in range(4):
                out[x, line : line + 64, :] = total
    mine, other = sketch_in[...], other_in[...]
    block = dot(mine, mine, ((0,), (0,)))
    cross[0] = dot(other, mine, ((0,), (0,)))
    cross[1] = dot(mine, other, ((0,), (0,)))
    half = cross[core, pl.ds(pl.multiple_of(64 * core, 64), 64), :]
    for start, part in ((0, block), (128, half)):
        size = part.shape[0]
        for line, piece in zip((576 + start, 768 + start), split(part)):
            for x in range(4):
                out[x, line : line + size, :] = piece
    for x in range(4):
        out[x, 960:984, :] = own[...]


def middle_kernel(pieces, out):
    total = (pieces[0, :960].astype(F32) + pieces[1, :960].astype(F32)) + (
        pieces[2, :960].astype(F32) + pieces[3, :960].astype(F32)
    )
    value, gram = split(total[:576]), split(total[576:768] + total[768:960])
    for core in range(2):
        out[core, :576, :] = value[0]
        out[core, 576:1152, :] = value[1]
        out[core, 1152:1344, :] = gram[0]
        out[core, 1344:1536, :] = gram[1]
        for x in range(4):
            out[core, 1536 + 24 * x : 1560 + 24 * x, :] = pieces[x, 960:984, :]


def split(value):
    high = value.astype(BF16)
    return high, (value - high.astype(F32)).astype(BF16)


def small_inverse(block):
    shape = (8, 8, 128)
    row, lane = 8 * iota(shape, 0) + iota(shape, 1), iota(shape, 2)
    work = jnp.where(lane < 64, block.reshape(shape), jnp.where(lane - 64 == row, 1.0, 0.0))
    for k in range(0, 64, 8):
        lines = [jnp.broadcast_to(work[k // 8, i : i + 1, :], (8, 128)) for i in range(8)]
        sides = [jnp.broadcast_to(work[:, :, k + j : k + j + 1], shape) for j in range(8)]
        corner = [[jnp.broadcast_to(sides[j][k // 8, i : i + 1, :], (8, 128)) for j in range(8)] for i in range(8)]
        update = jnp.zeros(shape, F32)
        for i in range(8):
            inverse = 1.0 / corner[i][i]
            update = update + jnp.where(row > k + i, sides[i], 0.0) * (lines[i] * inverse)
            for j in range(i + 1, 8):
                right = corner[i][j] * inverse
                below = corner[j][i] * inverse
                sides[j] = sides[j] - sides[i] * right
                lines[j] = lines[j] - below * lines[i]
                for m in range(i + 1, 8):
                    corner[j][m] = corner[j][m] - below * corner[i][m]
        work = work - update
    pivots = jnp.sum(jnp.where(lane == row, work, 0.0), axis=2, keepdims=True)
    return (work * lax.rsqrt(pivots)).reshape(64, 128)[:, 64:128]


def last_kernel(pieces, right, basis_out, block_out, gram, rest, inverse, sketch, value, result):
    for core in range(2):
        whole = pieces[core, 1152:1344, :].astype(F32) + pieces[core, 1344:1536, :].astype(F32)
        gram[128 * core : 128 * core + 128, 128 * core : 128 * core + 128] = whole[:128]
        gram[128 + 64 * core : 192 + 64 * core, :128] = whole[128:]
    gram[:128, 128:] = gram[128:, :128].T
    rest[...] = jnp.where(iota((256, 256), 0) == iota((256, 256), 1), 1.0, 0.0)
    inverse[...] = jnp.zeros((256, 256), F32)
    for step in range(4):
        top, tile = 64 * step, 128 * (step // 2)
        ahead, behind = (tile if step % 2 == 0 else 128), tile + 128
        block = gram[top : top + 64, tile : tile + 128]
        small = small_inverse(pltpu.roll(block, 64, 1) if step % 2 else block)
        lines = rest[top : top + 64, :behind]
        if step < 3:
            lines = jnp.concatenate([gram[top : top + 64, ahead:], lines], axis=1)
        lines = dot(small, lines, precision=HIGHEST)
        inverse[top : top + 64, :behind] = lines[:, lines.shape[1] - behind :]
        if step < 3:
            below = dot(lines[:, : 256 - ahead], lines, ((0,), (0,)), precision=HIGHEST)[top + 64 - ahead :]
            gram[top + 64 :, ahead:] = gram[top + 64 :, ahead:] - below[:, : 256 - ahead]
            rest[top + 64 :, :behind] = rest[top + 64 :, :behind] - below[:, 256 - ahead :]
    for core in range(2):
        for x in range(4):
            rows = pieces[core, 1536 + 24 * x : 1560 + 24 * x, :].astype(F32)
            sketch[18 * x : 18 * x + 18, 128 * core : 128 * core + 128] = rows[:18]
    high, low = split(inverse[...])
    own = sketch[...].astype(BF16)
    basis_out[...] = dot(own, high, ((1,), (1,))) + dot(own, low, ((1,), (1,)))
    for part in range(2):
        for core in range(2):
            lanes = slice(128 * core, 128 * core + 128)
            for tp in range(3):
                for t in range(3):
                    line = 576 * part + 64 * (3 * tp + t)
                    value[part, t, 64 * tp : 64 * tp + 64, lanes] = pieces[core, line : line + 64, :]
    wide = right[...].reshape(192, 512)
    for t in range(3):
        mixed = dot(high, value[0, t], ((1,), (1,))) + dot(low, value[0, t], ((1,), (1,)))
        mixed = mixed + dot(high, value[1, t], ((1,), (1,)))
        first, second = split(mixed)
        result[:, 512 * t : 512 * t + 512] = dot(first, wide) + dot(second, wide)
    upper = iota((8, 768), 0) < 4
    for pair in range(ROWS // 2):
        first = result[8 * pair : 8 * pair + 8, :768]
        second = result[8 * pair : 8 * pair + 8, 768:]
        block_out[2 * pair] = jnp.where(upper, first, pltpu.roll(second, 4, 0)).astype(BF16)
        block_out[2 * pair + 1] = jnp.where(upper, pltpu.roll(first, 4, 0), second).astype(BF16)


def block_kernel(pieces, out):
    total = jnp.sum(pieces[...].astype(F32), axis=0)
    picks = [stride_three(t, False) for t in range(3)]
    for j in range(4):
        lines = jnp.zeros((4, 384), F32)
        for t in range(3):
            start = 512 * t + 128 * j
            half, start = start // 768, start % 768
            rest = total[:, start : start + 128]
            spread = jnp.zeros((8, 384), F32)
            for _ in range(3):
                part = rest.astype(BF16)
                spread = spread + dot(part, picks[t])
                rest = rest - part.astype(F32)
            lines = lines + spread[4 * half : 4 * half + 4]
        out[:, 384 * j : 384 * j + 384] = lines


SMEM = pl.BlockSpec(memory_space=pltpu.SMEM)
VMEM = pl.BlockSpec(memory_space=pltpu.VMEM)
INTERPRET = False


def call(kernel, out, *args, smem=0, scratch=()):
    return pl.pallas_call(
        kernel,
        out_shape=[jax.ShapeDtypeStruct(*o) for o in out],
        in_specs=[SMEM] * smem + [VMEM] * (len(args) - smem),
        out_specs=[VMEM] * len(out),
        scratch_shapes=[pltpu.VMEM(*s) for s in scratch],
        compiler_params=pltpu.CompilerParams(vmem_limit_bytes=48 * 1024 * 1024),
        interpret=INTERPRET,
    )(*args)


PAIRS = [[0, 1], [2, 3], [4, 5], [6, 7]]
LINES_OF_X = [[0, 2, 4, 6], [1, 3, 5, 7]]


def exchange(value, axis, groups=None):
    return lax.all_to_all(value, axis, 0, 0, axis_index_groups=groups)


def exchange_lines(value, lines):
    return exchange(value.reshape(ROWS, lines // 2, 2, 128), "row").reshape(ROWS * lines, 128)


def local(left_site, right_site, gate, probes_matrix):
    place = jnp.stack([lax.axis_index("row"), lax.axis_index("col")]).astype(jnp.int32)
    left = left_site.transpose(1, 0, 2)
    right = right_site.transpose(1, 0, 2)
    (left_out,) = call(left_kernel, [((ROWS * 10, 128), BF16)], place, left, smem=1, scratch=[((ROWS * 10, 128), F32)])
    left_in = exchange_lines(left_out, 10)
    (weight,) = call(
        first_kernel,
        [((2, 192, 384), F32)],
        gate, right, probes_matrix,
        smem=1,
        scratch=[((3, 192, 256), F32)],
    )
    weight, left_in = lax.optimization_barrier((weight, left_in))
    weight = exchange(weight, "col", PAIRS)
    (weight,) = call(weight_kernel, [((4, 192, 384), BF16)], weight)
    weight = exchange(weight, "col", LINES_OF_X)
    sketch, left_rows = call(
        sketch_kernel,
        [((ROWS * 18, 128), BF16), ((384, 384), BF16)],
        left_in, weight,
        scratch=[((ROWS * 10, 128), F32), ((384, 384), BF16), ((384, 384), BF16), ((ROWS * 18, 128), F32)],
    )
    sketch = exchange_lines(sketch, 18)
    own, sketch = call(
        total_kernel,
        [((24, 128), BF16), ((ROWS * 18, 128), BF16)],
        sketch,
        scratch=[((72, 128), F32), ((144, 128), F32)],
    )
    sketch = exchange_lines(sketch, 18)
    other = lax.ppermute(sketch, "col", [(q, q ^ 1) for q in range(COLS)])
    (value,) = call(
        projection_kernel,
        [((4, 984, 128), BF16)],
        place, gate, sketch, other, left_rows, own,
        smem=2,
        scratch=[((ROWS * 18, 128), F32), ((384, 384), BF16), ((192, 384), F32), ((2, 128, 128), F32)],
    )
    value = exchange(value, "col", LINES_OF_X)
    (value,) = call(middle_kernel, [((2, 1632, 128), BF16)], value)
    value = exchange(value, "col", PAIRS)
    basis, block = call(
        last_kernel,
        [((72, 256), F32), ((ROWS, 8, 768), BF16)],
        value, right,
        scratch=[
            ((256, 256), F32), ((256, 256), F32), ((256, 256), F32), ((72, 256), F32),
            ((2, 3, 192, 256), BF16), ((256, 1536), F32),
        ],
    )
    block = exchange(block, "row")
    (new_block,) = call(block_kernel, [((4, 1536), F32)], block)
    return basis, new_block


def solution(mesh):
    return jax.shard_map(
        local,
        mesh=mesh,
        in_specs=(P("row", None, None), P("row", None, "col"), P(), P("col", None)),
        out_specs=(P("row", None), P("row", "col")),
        check_vma=False,
    )
```

```python
import jax
import jax.numpy as jnp
from jax import lax
from jax.experimental import pallas as pl
from jax.experimental.pallas import tpu as pltpu
from jax.sharding import PartitionSpec as P


F32 = jnp.float32
BF16 = jnp.bfloat16
HIGHEST = lax.Precision.HIGHEST
ROWS = 64
COLS = 8


def iota(shape, axis):
    return lax.broadcasted_iota(jnp.int32, shape, axis)


def dot(a, b, dims=((1,), (0,)), precision=None):
    return lax.dot_general(a, b, (dims, ((), ())), precision=precision, preferred_element_type=F32)


def stride_three(t, transposed):
    shape = (384, 128) if transposed else (128, 384)
    b, column = iota(shape, int(transposed)), iota(shape, int(not transposed))
    return jnp.where(column == 3 * b + t, 1.0, 0.0).astype(BF16)


def left_kernel(place, left, left_out, lines):
    row, column, lane = iota((16, 72), 0), iota((16, 72), 1), iota((16, 128), 1)
    sides = []
    for h in range(2):
        line = 2 * row + h
        photon = jnp.where(line < 6, 0, jnp.where(line < 12, 1, 2))
        chosen = (column == photon * 24 + 6 * (place[1] // 2) + line - 6 * photon) & (line < 18)
        sides.append(dot(jnp.where(chosen, 1.0, 0.0).astype(BF16), left[...].reshape(72, 4096)))
    for pair in range(ROWS // 2):
        even, odd = (side[:, 128 * pair : 128 * pair + 128] for side in sides)
        first = jnp.where(lane < 64, even, pltpu.roll(odd, 64, 1))
        second = jnp.where(lane < 64, pltpu.roll(even, 64, 1), odd)
        lines[20 * pair : 20 * pair + 10, :] = first[:10]
        lines[20 * pair + 10 : 20 * pair + 20, :] = second[:10]
    left_out[...] = lines[...].astype(BF16)


def first_kernel(place, gate, right, probes, right_other, probes_other, weight_out, product):
    half = pl.ds(pl.multiple_of(128 * (place[1] % 2), 128), 128)
    for t in range(3):
        pick = stride_three(t, False)
        total = jnp.zeros((192, 128), F32)
        for side, probe in ((right, probes), (right_other, probes_other)):
            own = [dot(pick, probe[384 * j : 384 * j + 384, half]).astype(BF16) for j in range(4)]
            total = total + dot(side[...].reshape(192, 512), jnp.concatenate(own, axis=0))
        product[t] = total
    for up in range(3):
        for s in range(3):
            total = jnp.zeros((64, 128), F32)
            for tp in range(3):
                for t in range(3):
                    total = total + gate[3 * s + t, 3 * up + tp] * product[t, 64 * tp : 64 * tp + 64, :]
            total = total.astype(BF16)
            for x in range(4):
                weight_out[x, 64 * up : 64 * up + 64, 128 * s : 128 * s + 128] = total


def sketch_kernel(left_in, weight, sketch_out, left_rows, wide_left, high, low, wide_sketch):
    wide_left[...] = left_in[...].astype(F32)
    side = iota((64, 128), 1) // 64
    for up in range(3):
        for i in range(6):
            line = 6 * up + i
            tile = jnp.where(side == line % 2, wide_left[pl.ds(line // 2, 64, stride=10), :], 0.0)
            left_rows[64 * i : 64 * i + 64, 128 * up : 128 * up + 128] = tile.astype(BF16)
    total = (weight[0].astype(F32) + weight[1].astype(F32)) + (weight[2].astype(F32) + weight[3].astype(F32))
    for part, wide in zip(split(total), (high, low)):
        for up in range(3):
            block = part[64 * up : 64 * up + 64]
            wide[128 * up : 128 * up + 64, :] = block
            wide[128 * up + 64 : 128 * up + 128, :] = block
    for i in range(6):
        rows = left_rows[64 * i : 64 * i + 64, :]
        part = dot(rows, high[...]) + dot(rows, low[...])
        for s in range(3):
            wide_sketch[pl.ds(3 * i + s, 64, stride=18), :] = part[:, 128 * s : 128 * s + 128]
    sketch_out[...] = wide_sketch[...].astype(BF16)


def total_kernel(pieces, own, out, four, many):
    total = pieces[:144, :].astype(F32)
    for k in range(1, 8):
        total = total + pieces[144 * k : 144 * k + 144, :].astype(F32)
    four[...] = total[:72] + total[72:]
    total = four[0:18, :] + four[18:36, :] + four[36:54, :] + four[54:72, :]
    own[:18, :] = total.astype(BF16)
    own[18:, :] = jnp.zeros((6, 128), BF16)
    for k in range(8):
        many[18 * k : 18 * k + 18, :] = total
    total = many[...].astype(BF16)
    for k in range(8):
        out[144 * k : 144 * k + 144, :] = total


def value_kernel(gate, sketch_in, left_rows, out, wide_sketch, sketch, product):
    wide_sketch[...] = sketch_in[...].astype(F32)
    for i in range(6):
        for s in range(3):
            tile = wide_sketch[pl.ds(3 * i + s, 64, stride=18), :]
            sketch[64 * i : 64 * i + 64, 128 * s : 128 * s + 128] = tile.astype(BF16)
    for up in range(3):
        part = dot(left_rows[:, 128 * up : 128 * up + 128], sketch[...], ((0,), (0,)))
        product[64 * up : 64 * up + 64, :] = part[:64] + part[64:]
    for tp in range(3):
        for t in range(3):
            total = jnp.zeros((64, 128), F32)
            for up in range(3):
                for s in range(3):
                    part = product[64 * up : 64 * up + 64, 128 * s : 128 * s + 128]
                    total = total + gate[3 * s + t, 3 * up + tp] * part
            line = 64 * (3 * tp + t)
            out[line : line + 64, :] = total.astype(BF16)


def gram_kernel(place, sketch_in, other_in, value, own, out, cross):
    core = place[1] % 2
    mine, other = sketch_in[...], other_in[...]
    block = dot(mine, mine, ((0,), (0,)))
    cross[0] = dot(other, mine, ((0,), (0,)))
    cross[1] = dot(mine, other, ((0,), (0,)))
    half = cross[core, pl.ds(pl.multiple_of(64 * core, 64), 64), :]
    block, half = split(block), split(half)
    for x in range(4):
        out[x, :576, :] = value[...]
        for part in range(2):
            out[x, 576 + 192 * part : 704 + 192 * part, :] = block[part]
            out[x, 704 + 192 * part : 768 + 192 * part, :] = half[part]
        out[x, 960:984, :] = own[...]


def middle_kernel(pieces, out):
    total = (pieces[0, :960].astype(F32) + pieces[1, :960].astype(F32)) + (
        pieces[2, :960].astype(F32) + pieces[3, :960].astype(F32)
    )
    value, gram = split(total[:576]), split(total[576:768] + total[768:960])
    for core in range(2):
        out[core, :576, :] = value[0]
        out[core, 576:1152, :] = value[1]
        out[core, 1152:1344, :] = gram[0]
        out[core, 1344:1536, :] = gram[1]
        for x in range(4):
            out[core, 1536 + 24 * x : 1560 + 24 * x, :] = pieces[x, 960:984, :]


def split(value):
    high = value.astype(BF16)
    return high, (value - high.astype(F32)).astype(BF16)


def small_inverse(block):
    shape = (8, 8, 128)
    row, lane = 8 * iota(shape, 0) + iota(shape, 1), iota(shape, 2)
    work = jnp.where(lane < 64, block.reshape(shape), jnp.where(lane - 64 == row, 1.0, 0.0))
    for k in range(0, 64, 8):
        lines = [jnp.broadcast_to(work[k // 8, i : i + 1, :], (8, 128)) for i in range(8)]
        sides = [jnp.broadcast_to(work[:, :, k + j : k + j + 1], shape) for j in range(8)]
        corner = [[jnp.broadcast_to(sides[j][k // 8, i : i + 1, :], (8, 128)) for j in range(8)] for i in range(8)]
        update = jnp.zeros(shape, F32)
        for i in range(8):
            inverse = 1.0 / corner[i][i]
            update = update + jnp.where(row > k + i, sides[i], 0.0) * (lines[i] * inverse)
            for j in range(i + 1, 8):
                right = corner[i][j] * inverse
                below = corner[j][i] * inverse
                sides[j] = sides[j] - sides[i] * right
                lines[j] = lines[j] - below * lines[i]
                for m in range(i + 1, 8):
                    corner[j][m] = corner[j][m] - below * corner[i][m]
        work = work - update
    pivots = jnp.sum(jnp.where(lane == row, work, 0.0), axis=2, keepdims=True)
    return (work * lax.rsqrt(pivots)).reshape(64, 128)[:, 64:128]


def last_kernel(pieces, right, basis_out, block_out, gram, rest, inverse, sketch, value, result):
    for core in range(2):
        whole = pieces[core, 1152:1344, :].astype(F32) + pieces[core, 1344:1536, :].astype(F32)
        gram[128 * core : 128 * core + 128, 128 * core : 128 * core + 128] = whole[:128]
        gram[128 + 64 * core : 192 + 64 * core, :128] = whole[128:]
    gram[:128, 128:] = gram[128:, :128].T
    rest[...] = jnp.where(iota((256, 256), 0) == iota((256, 256), 1), 1.0, 0.0)
    inverse[...] = jnp.zeros((256, 256), F32)
    for step in range(4):
        top, tile = 64 * step, 128 * (step // 2)
        ahead, behind = (tile if step % 2 == 0 else 128), tile + 128
        block = gram[top : top + 64, tile : tile + 128]
        small = small_inverse(pltpu.roll(block, 64, 1) if step % 2 else block)
        lines = rest[top : top + 64, :behind]
        if step < 3:
            lines = jnp.concatenate([gram[top : top + 64, ahead:], lines], axis=1)
        lines = dot(small, lines, precision=HIGHEST)
        inverse[top : top + 64, :behind] = lines[:, lines.shape[1] - behind :]
        if step < 3:
            below = dot(lines[:, : 256 - ahead], lines, ((0,), (0,)), precision=HIGHEST)[top + 64 - ahead :]
            gram[top + 64 :, ahead:] = gram[top + 64 :, ahead:] - below[:, : 256 - ahead]
            rest[top + 64 :, :behind] = rest[top + 64 :, :behind] - below[:, 256 - ahead :]
    for core in range(2):
        for x in range(4):
            rows = pieces[core, 1536 + 24 * x : 1560 + 24 * x, :].astype(F32)
            sketch[18 * x : 18 * x + 18, 128 * core : 128 * core + 128] = rows[:18]
    high, low = split(inverse[...])
    own = sketch[...].astype(BF16)
    basis_out[...] = dot(own, high, ((1,), (1,))) + dot(own, low, ((1,), (1,)))
    for part in range(2):
        for core in range(2):
            lanes = slice(128 * core, 128 * core + 128)
            for tp in range(3):
                for t in range(3):
                    line = 576 * part + 64 * (3 * tp + t)
                    value[part, t, 64 * tp : 64 * tp + 64, lanes] = pieces[core, line : line + 64, :]
    wide = right[...].reshape(192, 512)
    for t in range(3):
        mixed = dot(high, value[0, t], ((1,), (1,))) + dot(low, value[0, t], ((1,), (1,)))
        mixed = mixed + dot(high, value[1, t], ((1,), (1,)))
        first, second = split(mixed)
        result[:, 512 * t : 512 * t + 512] = dot(first, wide) + dot(second, wide)
    upper = iota((8, 768), 0) < 4
    for pair in range(ROWS // 2):
        first = result[8 * pair : 8 * pair + 8, :768]
        second = result[8 * pair : 8 * pair + 8, 768:]
        block_out[2 * pair] = jnp.where(upper, first, pltpu.roll(second, 4, 0)).astype(BF16)
        block_out[2 * pair + 1] = jnp.where(upper, pltpu.roll(first, 4, 0), second).astype(BF16)


def block_kernel(pieces, out):
    total = jnp.sum(pieces[...].astype(F32), axis=0)
    picks = [stride_three(t, False) for t in range(3)]
    for j in range(4):
        lines = jnp.zeros((4, 384), F32)
        for t in range(3):
            start = 512 * t + 128 * j
            half, start = start // 768, start % 768
            rest = total[:, start : start + 128]
            spread = jnp.zeros((8, 384), F32)
            for _ in range(3):
                part = rest.astype(BF16)
                spread = spread + dot(part, picks[t])
                rest = rest - part.astype(F32)
            lines = lines + spread[4 * half : 4 * half + 4]
        out[:, 384 * j : 384 * j + 384] = lines


SMEM = pl.BlockSpec(memory_space=pltpu.SMEM)
VMEM = pl.BlockSpec(memory_space=pltpu.VMEM)
INTERPRET = False


def call(kernel, out, *args, smem=0, scratch=()):
    return pl.pallas_call(
        kernel,
        out_shape=[jax.ShapeDtypeStruct(*o) for o in out],
        in_specs=[SMEM] * smem + [VMEM] * (len(args) - smem),
        out_specs=[VMEM] * len(out),
        scratch_shapes=[pltpu.VMEM(*s) for s in scratch],
        compiler_params=pltpu.CompilerParams(vmem_limit_bytes=48 * 1024 * 1024),
        interpret=INTERPRET,
    )(*args)


PAIRS = [[0, 1], [2, 3], [4, 5], [6, 7]]
LINES_OF_X = [[0, 2, 4, 6], [1, 3, 5, 7]]


def exchange(value, axis, groups=None):
    return lax.all_to_all(value, axis, 0, 0, axis_index_groups=groups)


def exchange_lines(value, lines):
    return exchange(value.reshape(ROWS, lines // 2, 2, 128), "row").reshape(ROWS * lines, 128)


def swap(value):
    return lax.ppermute(value, "col", [(q, q ^ 1) for q in range(COLS)])


def local(left_site, right_site, gate, probes_matrix):
    place = jnp.stack([lax.axis_index("row"), lax.axis_index("col")]).astype(jnp.int32)
    left = left_site.transpose(1, 0, 2)
    right = right_site.transpose(1, 0, 2)
    (left_out,) = call(left_kernel, [((ROWS * 10, 128), BF16)], place, left, smem=1, scratch=[((ROWS * 10, 128), F32)])
    left_in = exchange_lines(left_out, 10)
    right_other = swap(right)
    probes_other = swap(probes_matrix)
    (weight,) = call(
        first_kernel,
        [((4, 192, 384), BF16)],
        place, gate, right, probes_matrix, right_other, probes_other,
        smem=2,
        scratch=[((3, 192, 128), F32)],
    )
    weight, left_in = lax.optimization_barrier((weight, left_in))
    weight = exchange(weight, "col", LINES_OF_X)
    sketch, left_rows = call(
        sketch_kernel,
        [((ROWS * 18, 128), BF16), ((384, 384), BF16)],
        left_in, weight,
        scratch=[((ROWS * 10, 128), F32), ((384, 384), BF16), ((384, 384), BF16), ((ROWS * 18, 128), F32)],
    )
    sketch = exchange_lines(sketch, 18)
    own, sketch = call(
        total_kernel,
        [((24, 128), BF16), ((ROWS * 18, 128), BF16)],
        sketch,
        scratch=[((72, 128), F32), ((144, 128), F32)],
    )
    sketch = exchange_lines(sketch, 18)
    other = swap(sketch)
    (value,) = call(
        value_kernel,
        [((576, 128), BF16)],
        gate, sketch, left_rows,
        smem=1,
        scratch=[((ROWS * 18, 128), F32), ((384, 384), BF16), ((192, 384), F32)],
    )
    (value,) = call(
        gram_kernel,
        [((4, 984, 128), BF16)],
        place, sketch, other, value, own,
        smem=1,
        scratch=[((2, 128, 128), F32)],
    )
    value = exchange(value, "col", LINES_OF_X)
    (value,) = call(middle_kernel, [((2, 1632, 128), BF16)], value)
    value = exchange(value, "col", PAIRS)
    basis, block = call(
        last_kernel,
        [((72, 256), F32), ((ROWS, 8, 768), BF16)],
        value, right,
        scratch=[
            ((256, 256), F32), ((256, 256), F32), ((256, 256), F32), ((72, 256), F32),
            ((2, 3, 192, 256), BF16), ((256, 1536), F32),
        ],
    )
    block = exchange(block, "row")
    (new_block,) = call(block_kernel, [((4, 1536), F32)], block)
    return basis, new_block


def solution(mesh):
    return jax.shard_map(
        local,
        mesh=mesh,
        in_specs=(P("row", None, None), P("row", None, "col"), P(), P("col", None)),
        out_specs=(P("row", None), P("row", "col")),
        check_vma=False,
    )
```

```python
import jax
import jax.numpy as jnp
from jax import lax
from jax.experimental import pallas as pl
from jax.experimental.pallas import tpu as pltpu
from jax.sharding import PartitionSpec as P


F32 = jnp.float32
BF16 = jnp.bfloat16
HIGHEST = lax.Precision.HIGHEST
ROWS = 64
COLS = 8


def iota(shape, axis):
    return lax.broadcasted_iota(jnp.int32, shape, axis)


def dot(a, b, dims=((1,), (0,)), precision=None):
    return lax.dot_general(a, b, (dims, ((), ())), precision=precision, preferred_element_type=F32)


def stride_three(t, transposed):
    shape = (384, 128) if transposed else (128, 384)
    b, column = iota(shape, int(transposed)), iota(shape, int(not transposed))
    return jnp.where(column == 3 * b + t, 1.0, 0.0).astype(BF16)


def left_kernel(place, left, left_out, rows, lines, arrived):
    x = place[1] // 2
    start = pl.multiple_of(8 * (x // 2), 8)
    copies = [
        pltpu.make_async_copy(
            left.at[:, pl.ds(start, 16), 1024 * part : 1024 * part + 1024],
            rows.at[part],
            arrived.at[part],
        )
        for part in range(4)
    ]
    for copy in copies:
        copy.start()
    row, column, lane = iota((16, 48), 0), iota((16, 48), 1), iota((16, 128), 1)
    picks = []
    for h in range(2):
        line = 2 * row + h
        photon = jnp.where(line < 6, 0, jnp.where(line < 12, 1, 2))
        chosen = (column == photon * 16 + 6 * x - start + line - 6 * photon) & (line < 18)
        picks.append(jnp.where(chosen, 1.0, 0.0).astype(BF16))
    for part in range(4):
        copies[part].wait()
        sides = [dot(pick, rows[part].reshape(48, 1024)) for pick in picks]
        for pair in range(8):
            even, odd = (side[:, 128 * pair : 128 * pair + 128] for side in sides)
            first = jnp.where(lane < 64, even, pltpu.roll(odd, 64, 1))
            second = jnp.where(lane < 64, pltpu.roll(even, 64, 1), odd)
            at = 160 * part + 20 * pair
            lines[at : at + 10, :] = first[:10]
            lines[at + 10 : at + 20, :] = second[:10]
    left_out[...] = lines[...].astype(BF16)


def first_kernel(place, gate, right, probes, right_other, probes_other, weight_out, product):
    half = pl.ds(pl.multiple_of(128 * (place[1] % 2), 128), 128)
    for t in range(3):
        pick = stride_three(t, False)
        total = jnp.zeros((192, 128), F32)
        for side, probe in ((right, probes), (right_other, probes_other)):
            own = [dot(pick, probe[384 * j : 384 * j + 384, half]).astype(BF16) for j in range(4)]
            total = total + dot(side[...].reshape(192, 512), jnp.concatenate(own, axis=0))
        product[t] = total
    for up in range(3):
        for s in range(3):
            total = jnp.zeros((64, 128), F32)
            for tp in range(3):
                for t in range(3):
                    total = total + gate[3 * s + t, 3 * up + tp] * product[t, 64 * tp : 64 * tp + 64, :]
            total = total.astype(BF16)
            for x in range(4):
                weight_out[x, 64 * up : 64 * up + 64, 128 * s : 128 * s + 128] = total


def sketch_kernel(left_in, weight, sketch_out, left_rows, wide_left, high, low, wide_sketch):
    wide_left[...] = left_in[...].astype(F32)
    side = iota((64, 128), 1) // 64
    for up in range(3):
        for i in range(6):
            line = 6 * up + i
            tile = jnp.where(side == line % 2, wide_left[pl.ds(line // 2, 64, stride=10), :], 0.0)
            left_rows[64 * i : 64 * i + 64, 128 * up : 128 * up + 128] = tile.astype(BF16)
    total = (weight[0].astype(F32) + weight[1].astype(F32)) + (weight[2].astype(F32) + weight[3].astype(F32))
    for part, wide in zip(split(total), (high, low)):
        for up in range(3):
            block = part[64 * up : 64 * up + 64]
            wide[128 * up : 128 * up + 64, :] = block
            wide[128 * up + 64 : 128 * up + 128, :] = block
    for i in range(6):
        rows = left_rows[64 * i : 64 * i + 64, :]
        part = dot(rows, high[...]) + dot(rows, low[...])
        for s in range(3):
            wide_sketch[pl.ds(3 * i + s, 64, stride=18), :] = part[:, 128 * s : 128 * s + 128]
    sketch_out[...] = wide_sketch[...].astype(BF16)


def total_kernel(pieces, own, out, four, many):
    total = pieces[:144, :].astype(F32)
    for k in range(1, 8):
        total = total + pieces[144 * k : 144 * k + 144, :].astype(F32)
    four[...] = total[:72] + total[72:]
    total = four[0:18, :] + four[18:36, :] + four[36:54, :] + four[54:72, :]
    own[:18, :] = total.astype(BF16)
    own[18:, :] = jnp.zeros((6, 128), BF16)
    for k in range(8):
        many[18 * k : 18 * k + 18, :] = total
    total = many[...].astype(BF16)
    for k in range(8):
        out[144 * k : 144 * k + 144, :] = total


def value_kernel(gate, sketch_in, left_rows, out, wide_sketch, sketch, product):
    wide_sketch[...] = sketch_in[...].astype(F32)
    for i in range(6):
        for s in range(3):
            tile = wide_sketch[pl.ds(3 * i + s, 64, stride=18), :]
            sketch[64 * i : 64 * i + 64, 128 * s : 128 * s + 128] = tile.astype(BF16)
    for up in range(3):
        part = dot(left_rows[:, 128 * up : 128 * up + 128], sketch[...], ((0,), (0,)))
        product[64 * up : 64 * up + 64, :] = part[:64] + part[64:]
    for tp in range(3):
        for t in range(3):
            total = jnp.zeros((64, 128), F32)
            for up in range(3):
                for s in range(3):
                    part = product[64 * up : 64 * up + 64, 128 * s : 128 * s + 128]
                    total = total + gate[3 * s + t, 3 * up + tp] * part
            line = 64 * (3 * tp + t)
            out[line : line + 64, :] = total.astype(BF16)


def gram_kernel(place, sketch_in, other_in, value, own, out, cross):
    core = place[1] % 2
    mine, other = sketch_in[...], other_in[...]
    block = dot(mine, mine, ((0,), (0,)))
    cross[0] = dot(other, mine, ((0,), (0,)))
    cross[1] = dot(mine, other, ((0,), (0,)))
    half = cross[core, pl.ds(pl.multiple_of(64 * core, 64), 64), :]
    block, half = split(block), split(half)
    for x in range(4):
        out[x, :576, :] = value[...]
        for part in range(2):
            out[x, 576 + 192 * part : 704 + 192 * part, :] = block[part]
            out[x, 704 + 192 * part : 768 + 192 * part, :] = half[part]
        out[x, 960:984, :] = own[...]


def middle_kernel(pieces, out):
    total = (pieces[0, :960].astype(F32) + pieces[1, :960].astype(F32)) + (
        pieces[2, :960].astype(F32) + pieces[3, :960].astype(F32)
    )
    value, gram = split(total[:576]), split(total[576:768] + total[768:960])
    out[:576, :] = value[0]
    out[576:1152, :] = value[1]
    out[1152:1344, :] = gram[0]
    out[1344:1536, :] = gram[1]
    for x in range(4):
        out[1536 + 24 * x : 1560 + 24 * x, :] = pieces[x, 960:984, :]


def split(value):
    high = value.astype(BF16)
    return high, (value - high.astype(F32)).astype(BF16)


def small_inverse(block):
    row, lane, sub = iota((64, 128), 0), iota((64, 128), 1), iota((8, 128), 0)
    diagonal = jnp.where(lane == row, block, 0.0)
    tall = lax.rsqrt(jnp.sum(diagonal, axis=1, keepdims=True))
    flat = jnp.sum(diagonal, axis=0, keepdims=True)
    flat = lax.rsqrt(jnp.where(iota((1, 128), 1) < 64, flat, 1.0))
    tail = jnp.where(lane < 64, block * tall * flat, jnp.where(lane - 64 == row, 1.0, 0.0)).reshape(8, 8, 128)
    done = []
    for k in range(0, 64, 8):
        head, tail = tail[0], tail[1:]
        count = tail.shape[0]
        lines = [jnp.broadcast_to(head[i : i + 1, :], (8, 128)) for i in range(8)]
        corner = [
            [jnp.broadcast_to(lines[i][:, k + j : k + j + 1], (8, 128)) if j >= i else None for j in range(8)]
            for i in range(8)
        ]
        if count:
            sides = [jnp.broadcast_to(tail[:, :, k + j : k + j + 1], tail.shape) for j in range(8)]
        for i in range(0, 8, 2):
            first, both, second = corner[i][i], corner[i][i + 1], corner[i + 1][i + 1]
            inverse = 1.0 / first
            ratio = both * inverse
            inverse_two = first * (1.0 / (first * second - both * both))
            lines[i + 1] = lines[i + 1] - ratio * lines[i]
            above, below = lines[i] * inverse, lines[i + 1] * inverse_two
            upper = corner[i]
            lower = [None if m <= i + 1 else corner[i + 1][m] - ratio * upper[m] for m in range(8)]
            if count:
                sides[i + 1] = sides[i + 1] - ratio * sides[i]
                tail = tail - (sides[i] * above + sides[i + 1] * below)
            for j in range(i + 2, 8):
                one, two = upper[j] * inverse, lower[j] * inverse_two
                lines[j] = lines[j] - (one * lines[i] + two * lines[i + 1])
                if count:
                    sides[j] = sides[j] - (one * sides[i] + two * sides[i + 1])
                for m in range(j, 8):
                    corner[j][m] = corner[j][m] - (one * upper[m] + two * lower[m])
        head = lines[7]
        for i in range(7):
            head = jnp.where(sub == i, lines[i], head)
        done.append(head)
    work = jnp.concatenate(done, axis=0)
    pivots = jnp.sum(jnp.where(lane == row, work, 0.0), axis=1, keepdims=True)
    return (work * lax.rsqrt(pivots))[:, 64:128] * flat[:, :64]


def last_kernel(place, mine, other, right, basis_out, block_out, gram, rest, inverse, sketch, value, result):
    core = place[1] % 2
    halves = [(side, pl.ds(pl.multiple_of(128 * k, 128), 128), k) for side, k in ((mine, core), (other, 1 - core))]
    for pieces, half, k in halves:
        whole = pieces[1152:1344, :].astype(F32) + pieces[1344:1536, :].astype(F32)
        gram[half, half] = whole[:128]
        gram[pl.ds(pl.multiple_of(128 + 64 * k, 64), 64), :128] = whole[128:]
    gram[:128, 128:] = gram[128:, :128].T
    rest[...] = jnp.where(iota((256, 256), 0) == iota((256, 256), 1), 1.0, 0.0)
    inverse[...] = jnp.zeros((256, 256), F32)
    for step in range(4):
        top, tile = 64 * step, 128 * (step // 2)
        ahead, behind = (tile if step % 2 == 0 else 128), tile + 128
        block = gram[top : top + 64, tile : tile + 128]
        small = small_inverse(pltpu.roll(block, 64, 1) if step % 2 else block)
        lines = rest[top : top + 64, :behind]
        if step < 3:
            lines = jnp.concatenate([gram[top : top + 64, ahead:], lines], axis=1)
        lines = dot(small, lines, precision=HIGHEST)
        inverse[top : top + 64, :behind] = lines[:, lines.shape[1] - behind :]
        if step < 3:
            below = dot(lines[:, : 256 - ahead], lines, ((0,), (0,)), precision=HIGHEST)[top + 64 - ahead :]
            gram[top + 64 :, ahead:] = gram[top + 64 :, ahead:] - below[:, : 256 - ahead]
            rest[top + 64 :, :behind] = rest[top + 64 :, :behind] - below[:, 256 - ahead :]
    for pieces, half, _ in halves:
        for x in range(4):
            rows = pieces[1536 + 24 * x : 1560 + 24 * x, :].astype(F32)
            sketch[18 * x : 18 * x + 18, half] = rows[:18]
    high, low = split(inverse[...])
    own = sketch[...].astype(BF16)
    basis_out[...] = dot(own, high, ((1,), (1,))) + dot(own, low, ((1,), (1,)))
    for part in range(2):
        for pieces, half, _ in halves:
            for tp in range(3):
                for t in range(3):
                    line = 576 * part + 64 * (3 * tp + t)
                    value[part, t, 64 * tp : 64 * tp + 64, half] = pieces[line : line + 64, :]
    wide = right[...].reshape(192, 512)
    for t in range(3):
        mixed = dot(high, value[0, t], ((1,), (1,))) + dot(low, value[0, t], ((1,), (1,)))
        mixed = mixed + dot(high, value[1, t], ((1,), (1,)))
        first, second = split(mixed)
        result[:, 512 * t : 512 * t + 512] = dot(first, wide) + dot(second, wide)
    upper = iota((8, 768), 0) < 4
    for pair in range(ROWS // 2):
        first = result[8 * pair : 8 * pair + 8, :768]
        second = result[8 * pair : 8 * pair + 8, 768:]
        block_out[2 * pair] = jnp.where(upper, first, pltpu.roll(second, 4, 0)).astype(BF16)
        block_out[2 * pair + 1] = jnp.where(upper, pltpu.roll(first, 4, 0), second).astype(BF16)


def block_kernel(pieces, out):
    total = jnp.sum(pieces[...].astype(F32), axis=0)
    picks = [stride_three(t, False) for t in range(3)]
    for j in range(4):
        lines = jnp.zeros((4, 384), F32)
        for t in range(3):
            start = 512 * t + 128 * j
            half, start = start // 768, start % 768
            rest = total[:, start : start + 128]
            spread = jnp.zeros((8, 384), F32)
            for _ in range(3):
                part = rest.astype(BF16)
                spread = spread + dot(part, picks[t])
                rest = rest - part.astype(F32)
            lines = lines + spread[4 * half : 4 * half + 4]
        out[:, 384 * j : 384 * j + 384] = lines


SMEM = pl.BlockSpec(memory_space=pltpu.SMEM)
VMEM = pl.BlockSpec(memory_space=pltpu.VMEM)
INTERPRET = False


def call(kernel, out, *args, smem=0, far=0, scratch=(), copies=0):
    near = len(args) - smem - far
    shapes = [pltpu.VMEM(*s) for s in scratch]
    return pl.pallas_call(
        kernel,
        out_shape=[jax.ShapeDtypeStruct(*o) for o in out],
        in_specs=[SMEM] * smem + [VMEM] * near + [pl.BlockSpec(memory_space=pltpu.HBM)] * far,
        out_specs=[VMEM] * len(out),
        scratch_shapes=shapes + ([pltpu.SemaphoreType.DMA((copies,))] if copies else []),
        compiler_params=pltpu.CompilerParams(vmem_limit_bytes=48 * 1024 * 1024),
        interpret=INTERPRET,
    )(*args)


LINES_OF_X = [[0, 2, 4, 6], [1, 3, 5, 7]]


def exchange(value, axis, groups=None):
    return lax.all_to_all(value, axis, 0, 0, axis_index_groups=groups)


def exchange_lines(value, lines):
    return exchange(value.reshape(ROWS, lines // 2, 2, 128), "row").reshape(ROWS * lines, 128)


def swap(value):
    return lax.ppermute(value, "col", [(q, q ^ 1) for q in range(COLS)])


def local(left_site, right_site, gate, probes_matrix):
    place = jnp.stack([lax.axis_index("row"), lax.axis_index("col")]).astype(jnp.int32)
    left = left_site.transpose(1, 0, 2)
    right = right_site.transpose(1, 0, 2)
    (left_out,) = call(
        left_kernel,
        [((ROWS * 10, 128), BF16)],
        place, pltpu.with_memory_space_constraint(left, pltpu.HBM),
        smem=1,
        far=1,
        scratch=[((4, 3, 16, 1024), BF16), ((ROWS * 10, 128), F32)],
        copies=4,
    )
    left_in = exchange_lines(left_out, 10)
    right_other = swap(right)
    probes_other = swap(probes_matrix)
    (weight,) = call(
        first_kernel,
        [((4, 192, 384), BF16)],
        place, gate, right, probes_matrix, right_other, probes_other,
        smem=2,
        scratch=[((3, 192, 128), F32)],
    )
    weight, left_in = lax.optimization_barrier((weight, left_in))
    weight = exchange(weight, "col", LINES_OF_X)
    sketch, left_rows = call(
        sketch_kernel,
        [((ROWS * 18, 128), BF16), ((384, 384), BF16)],
        left_in, weight,
        scratch=[((ROWS * 10, 128), F32), ((384, 384), BF16), ((384, 384), BF16), ((ROWS * 18, 128), F32)],
    )
    sketch = exchange_lines(sketch, 18)
    own, sketch = call(
        total_kernel,
        [((24, 128), BF16), ((ROWS * 18, 128), BF16)],
        sketch,
        scratch=[((72, 128), F32), ((144, 128), F32)],
    )
    sketch = exchange_lines(sketch, 18)
    other = swap(sketch)
    (value,) = call(
        value_kernel,
        [((576, 128), BF16)],
        gate, sketch, left_rows,
        smem=1,
        scratch=[((ROWS * 18, 128), F32), ((384, 384), BF16), ((192, 384), F32)],
    )
    (value,) = call(
        gram_kernel,
        [((4, 984, 128), BF16)],
        place, sketch, other, value, own,
        smem=1,
        scratch=[((2, 128, 128), F32)],
    )
    value = exchange(value, "col", LINES_OF_X)
    (value,) = call(middle_kernel, [((1632, 128), BF16)], value)
    basis, block = call(
        last_kernel,
        [((72, 256), F32), ((ROWS, 8, 768), BF16)],
        place, value, swap(value), right,
        smem=1,
        scratch=[
            ((256, 256), F32), ((256, 256), F32), ((256, 256), F32), ((72, 256), F32),
            ((2, 3, 192, 256), BF16), ((256, 1536), F32),
        ],
    )
    block = exchange(block, "row")
    (new_block,) = call(block_kernel, [((4, 1536), F32)], block)
    return basis, new_block


def solution(mesh):
    return jax.shard_map(
        local,
        mesh=mesh,
        in_specs=(P("row", None, None), P("row", None, "col"), P(), P("col", None)),
        out_specs=(P("row", None), P("row", "col")),
        check_vma=False,
    )
```

```python
import jax
import jax.numpy as jnp
from jax import lax
from jax.experimental import pallas as pl
from jax.experimental.pallas import tpu as pltpu
from jax.sharding import PartitionSpec as P


F32 = jnp.float32
BF16 = jnp.bfloat16
HIGHEST = lax.Precision.HIGHEST
ROWS = 64
COLS = 8


def iota(shape, axis):
    return lax.broadcasted_iota(jnp.int32, shape, axis)


def dot(a, b, dims=((1,), (0,)), precision=None):
    return lax.dot_general(a, b, (dims, ((), ())), precision=precision, preferred_element_type=F32)


def stride_three(t, transposed):
    shape = (384, 128) if transposed else (128, 384)
    b, column = iota(shape, int(transposed)), iota(shape, int(not transposed))
    return jnp.where(column == 3 * b + t, 1.0, 0.0).astype(BF16)


def left_kernel(place, left, left_out, lines):
    row, column, lane = iota((16, 72), 0), iota((16, 72), 1), iota((16, 128), 1)
    sides = []
    for h in range(2):
        line = 2 * row + h
        photon = jnp.where(line < 6, 0, jnp.where(line < 12, 1, 2))
        chosen = (column == photon * 24 + 6 * (place[1] // 2) + line - 6 * photon) & (line < 18)
        sides.append(dot(jnp.where(chosen, 1.0, 0.0).astype(BF16), left[...].reshape(72, 4096)))
    for pair in range(ROWS // 2):
        even, odd = (side[:, 128 * pair : 128 * pair + 128] for side in sides)
        first = jnp.where(lane < 64, even, pltpu.roll(odd, 64, 1))
        second = jnp.where(lane < 64, pltpu.roll(even, 64, 1), odd)
        lines[20 * pair : 20 * pair + 10, :] = first[:10]
        lines[20 * pair + 10 : 20 * pair + 20, :] = second[:10]
    left_out[...] = lines[...].astype(BF16)


def first_kernel(place, gate, right, probes, kept, sent, product):
    core = place[1] % 2
    wide = right[...].reshape(192, 512)
    for t in range(3):
        pick = stride_three(t, False)
        own = [dot(pick, probes[384 * j : 384 * j + 384, :]).astype(BF16) for j in range(4)]
        product[t] = dot(wide, jnp.concatenate(own, axis=0))
    for out, k in ((sent, 1 - core), (kept, core)):
        half = pl.ds(pl.multiple_of(128 * k, 128), 128)
        for up in range(3):
            for s in range(3):
                total = jnp.zeros((64, 128), F32)
                for tp in range(3):
                    for t in range(3):
                        total = total + gate[3 * s + t, 3 * up + tp] * product[t, 64 * tp : 64 * tp + 64, half]
                out[64 * up : 64 * up + 64, 128 * s : 128 * s + 128] = total


def weight_kernel(kept, received, out):
    total = (kept[...] + received[...]).astype(BF16)
    for x in range(4):
        out[x] = total


def sketch_kernel(left_in, weight, sketch_out, left_rows, wide_left, high, low, wide_sketch):
    wide_left[...] = left_in[...].astype(F32)
    side = iota((64, 128), 1) // 64
    for up in range(3):
        for i in range(6):
            line = 6 * up + i
            tile = jnp.where(side == line % 2, wide_left[pl.ds(line // 2, 64, stride=10), :], 0.0)
            left_rows[64 * i : 64 * i + 64, 128 * up : 128 * up + 128] = tile.astype(BF16)
    total = (weight[0].astype(F32) + weight[1].astype(F32)) + (weight[2].astype(F32) + weight[3].astype(F32))
    for part, wide in zip(split(total), (high, low)):
        for up in range(3):
            block = part[64 * up : 64 * up + 64]
            wide[128 * up : 128 * up + 64, :] = block
            wide[128 * up + 64 : 128 * up + 128, :] = block
    for i in range(6):
        rows = left_rows[64 * i : 64 * i + 64, :]
        part = dot(rows, high[...]) + dot(rows, low[...])
        for s in range(3):
            wide_sketch[pl.ds(3 * i + s, 64, stride=18), :] = part[:, 128 * s : 128 * s + 128]
    sketch_out[...] = wide_sketch[...].astype(BF16)


def total_kernel(pieces, own, out, four, many):
    total = pieces[:144, :].astype(F32)
    for k in range(1, 8):
        total = total + pieces[144 * k : 144 * k + 144, :].astype(F32)
    four[...] = total[:72] + total[72:]
    total = four[0:18, :] + four[18:36, :] + four[36:54, :] + four[54:72, :]
    own[:18, :] = total.astype(BF16)
    own[18:, :] = jnp.zeros((6, 128), BF16)
    for k in range(8):
        many[18 * k : 18 * k + 18, :] = total
    total = many[...].astype(BF16)
    for k in range(8):
        out[144 * k : 144 * k + 144, :] = total


def value_kernel(gate, sketch_in, left_rows, out, wide_sketch, sketch, product):
    wide_sketch[...] = sketch_in[...].astype(F32)
    for i in range(6):
        for s in range(3):
            tile = wide_sketch[pl.ds(3 * i + s, 64, stride=18), :]
            sketch[64 * i : 64 * i + 64, 128 * s : 128 * s + 128] = tile.astype(BF16)
    for up in range(3):
        part = dot(left_rows[:, 128 * up : 128 * up + 128], sketch[...], ((0,), (0,)))
        product[64 * up : 64 * up + 64, :] = part[:64] + part[64:]
    for tp in range(3):
        for t in range(3):
            total = jnp.zeros((64, 128), F32)
            for up in range(3):
                for s in range(3):
                    part = product[64 * up : 64 * up + 64, 128 * s : 128 * s + 128]
                    total = total + gate[3 * s + t, 3 * up + tp] * part
            line = 64 * (3 * tp + t)
            out[line : line + 64, :] = total.astype(BF16)


def gram_kernel(place, sketch_in, other_in, value, own, out, cross):
    core = place[1] % 2
    mine, other = sketch_in[...], other_in[...]
    block = dot(mine, mine, ((0,), (0,)))
    cross[0] = dot(other, mine, ((0,), (0,)))
    cross[1] = dot(mine, other, ((0,), (0,)))
    half = cross[core, pl.ds(pl.multiple_of(64 * core, 64), 64), :]
    block, half = split(block), split(half)
    for x in range(4):
        out[x, :576, :] = value[...]
        for part in range(2):
            out[x, 576 + 192 * part : 704 + 192 * part, :] = block[part]
            out[x, 704 + 192 * part : 768 + 192 * part, :] = half[part]
        out[x, 960:984, :] = own[...]


def middle_kernel(pieces, out):
    total = (pieces[0, :960].astype(F32) + pieces[1, :960].astype(F32)) + (
        pieces[2, :960].astype(F32) + pieces[3, :960].astype(F32)
    )
    value, gram = split(total[:576]), split(total[576:768] + total[768:960])
    out[:576, :] = value[0]
    out[576:1152, :] = value[1]
    out[1152:1344, :] = gram[0]
    out[1344:1536, :] = gram[1]
    for x in range(4):
        out[1536 + 24 * x : 1560 + 24 * x, :] = pieces[x, 960:984, :]


def split(value):
    high = value.astype(BF16)
    return high, (value - high.astype(F32)).astype(BF16)


def small_inverse(block):
    row, lane, sub = iota((64, 128), 0), iota((64, 128), 1), iota((8, 128), 0)
    diagonal = jnp.where(lane == row, block, 0.0)
    tall = lax.rsqrt(jnp.sum(diagonal, axis=1, keepdims=True))
    flat = jnp.sum(diagonal, axis=0, keepdims=True)
    flat = lax.rsqrt(jnp.where(iota((1, 128), 1) < 64, flat, 1.0))
    tail = jnp.where(lane < 64, block * tall * flat, jnp.where(lane - 64 == row, 1.0, 0.0)).reshape(8, 8, 128)
    done = []
    for k in range(0, 64, 8):
        head, tail = tail[0], tail[1:]
        count = tail.shape[0]
        lines = [jnp.broadcast_to(head[i : i + 1, :], (8, 128)) for i in range(8)]
        corner = [
            [jnp.broadcast_to(lines[i][:, k + j : k + j + 1], (8, 128)) if j >= i else None for j in range(8)]
            for i in range(8)
        ]
        if count:
            sides = [jnp.broadcast_to(tail[:, :, k + j : k + j + 1], tail.shape) for j in range(8)]
        for i in range(0, 8, 2):
            first, both, second = corner[i][i], corner[i][i + 1], corner[i + 1][i + 1]
            inverse = 1.0 / first
            ratio = both * inverse
            inverse_two = first * (1.0 / (first * second - both * both))
            lines[i + 1] = lines[i + 1] - ratio * lines[i]
            above, below = lines[i] * inverse, lines[i + 1] * inverse_two
            upper = corner[i]
            lower = [None if m <= i + 1 else corner[i + 1][m] - ratio * upper[m] for m in range(8)]
            if count:
                sides[i + 1] = sides[i + 1] - ratio * sides[i]
                tail = tail - (sides[i] * above + sides[i + 1] * below)
            for j in range(i + 2, 8):
                one, two = upper[j] * inverse, lower[j] * inverse_two
                lines[j] = lines[j] - (one * lines[i] + two * lines[i + 1])
                if count:
                    sides[j] = sides[j] - (one * sides[i] + two * sides[i + 1])
                for m in range(j, 8):
                    corner[j][m] = corner[j][m] - (one * upper[m] + two * lower[m])
        head = lines[7]
        for i in range(7):
            head = jnp.where(sub == i, lines[i], head)
        done.append(head)
    work = jnp.concatenate(done, axis=0)
    pivots = jnp.sum(jnp.where(lane == row, work, 0.0), axis=1, keepdims=True)
    return (work * lax.rsqrt(pivots))[:, 64:128] * flat[:, :64]


def last_kernel(place, mine, other, right, basis_out, block_out, gram, rest, inverse, sketch, value, result):
    core = place[1] % 2
    halves = [(side, pl.ds(pl.multiple_of(128 * k, 128), 128), k) for side, k in ((mine, core), (other, 1 - core))]
    for pieces, half, k in halves:
        whole = pieces[1152:1344, :].astype(F32) + pieces[1344:1536, :].astype(F32)
        gram[half, half] = whole[:128]
        gram[pl.ds(pl.multiple_of(128 + 64 * k, 64), 64), :128] = whole[128:]
    gram[:128, 128:] = gram[128:, :128].T
    rest[...] = jnp.where(iota((256, 256), 0) == iota((256, 256), 1), 1.0, 0.0)
    inverse[...] = jnp.zeros((256, 256), F32)
    for step in range(4):
        top, tile = 64 * step, 128 * (step // 2)
        ahead, behind = (tile if step % 2 == 0 else 128), tile + 128
        block = gram[top : top + 64, tile : tile + 128]
        small = small_inverse(pltpu.roll(block, 64, 1) if step % 2 else block)
        lines = rest[top : top + 64, :behind]
        if step < 3:
            lines = jnp.concatenate([gram[top : top + 64, ahead:], lines], axis=1)
        lines = dot(small, lines, precision=HIGHEST)
        inverse[top : top + 64, :behind] = lines[:, lines.shape[1] - behind :]
        if step < 3:
            below = dot(lines[:, : 256 - ahead], lines, ((0,), (0,)), precision=HIGHEST)[top + 64 - ahead :]
            gram[top + 64 :, ahead:] = gram[top + 64 :, ahead:] - below[:, : 256 - ahead]
            rest[top + 64 :, :behind] = rest[top + 64 :, :behind] - below[:, 256 - ahead :]
    for pieces, half, _ in halves:
        for x in range(4):
            rows = pieces[1536 + 24 * x : 1560 + 24 * x, :].astype(F32)
            sketch[18 * x : 18 * x + 18, half] = rows[:18]
    high, low = split(inverse[...])
    own = sketch[...].astype(BF16)
    basis_out[...] = dot(own, high, ((1,), (1,))) + dot(own, low, ((1,), (1,)))
    for part in range(2):
        for pieces, half, _ in halves:
            for tp in range(3):
                for t in range(3):
                    line = 576 * part + 64 * (3 * tp + t)
                    value[part, t, 64 * tp : 64 * tp + 64, half] = pieces[line : line + 64, :]
    wide = right[...].reshape(192, 512)
    for t in range(3):
        mixed = dot(high, value[0, t], ((1,), (1,))) + dot(low, value[0, t], ((1,), (1,)))
        mixed = mixed + dot(high, value[1, t], ((1,), (1,)))
        first, second = split(mixed)
        result[:, 512 * t : 512 * t + 512] = dot(first, wide) + dot(second, wide)
    upper = iota((8, 768), 0) < 4
    for pair in range(ROWS // 2):
        first = result[8 * pair : 8 * pair + 8, :768]
        second = result[8 * pair : 8 * pair + 8, 768:]
        block_out[2 * pair] = jnp.where(upper, first, pltpu.roll(second, 4, 0)).astype(BF16)
        block_out[2 * pair + 1] = jnp.where(upper, pltpu.roll(first, 4, 0), second).astype(BF16)


def block_kernel(pieces, out):
    total = jnp.sum(pieces[...].astype(F32), axis=0)
    picks = [stride_three(t, False) for t in range(3)]
    for j in range(4):
        lines = jnp.zeros((4, 384), F32)
        for t in range(3):
            start = 512 * t + 128 * j
            half, start = start // 768, start % 768
            rest = total[:, start : start + 128]
            spread = jnp.zeros((8, 384), F32)
            for _ in range(3):
                part = rest.astype(BF16)
                spread = spread + dot(part, picks[t])
                rest = rest - part.astype(F32)
            lines = lines + spread[4 * half : 4 * half + 4]
        out[:, 384 * j : 384 * j + 384] = lines


SMEM = pl.BlockSpec(memory_space=pltpu.SMEM)
VMEM = pl.BlockSpec(memory_space=pltpu.VMEM)
INTERPRET = False


def call(kernel, out, *args, smem=0, scratch=()):
    return pl.pallas_call(
        kernel,
        out_shape=[jax.ShapeDtypeStruct(*o) for o in out],
        in_specs=[SMEM] * smem + [VMEM] * (len(args) - smem),
        out_specs=[VMEM] * len(out),
        scratch_shapes=[pltpu.VMEM(*s) for s in scratch],
        compiler_params=pltpu.CompilerParams(vmem_limit_bytes=48 * 1024 * 1024),
        interpret=INTERPRET,
    )(*args)


LINES_OF_X = [[0, 2, 4, 6], [1, 3, 5, 7]]


def exchange(value, axis, groups=None):
    return lax.all_to_all(value, axis, 0, 0, axis_index_groups=groups)


def exchange_lines(value, lines):
    return exchange(value.reshape(ROWS, lines // 2, 2, 128), "row").reshape(ROWS * lines, 128)


def swap(value):
    return lax.ppermute(value, "col", [(q, q ^ 1) for q in range(COLS)])


def local(left_site, right_site, gate, probes_matrix):
    place = jnp.stack([lax.axis_index("row"), lax.axis_index("col")]).astype(jnp.int32)
    left = left_site.transpose(1, 0, 2)
    right = right_site.transpose(1, 0, 2)
    (left_out,) = call(left_kernel, [((ROWS * 10, 128), BF16)], place, left, smem=1, scratch=[((ROWS * 10, 128), F32)])
    left_in = exchange_lines(left_out, 10)
    kept, sent = call(
        first_kernel,
        [((192, 384), F32), ((192, 384), F32)],
        place, gate, right, probes_matrix,
        smem=2,
        scratch=[((3, 192, 256), F32)],
    )
    received = swap(sent)
    (weight,) = call(weight_kernel, [((4, 192, 384), BF16)], kept, received)
    weight, left_in = lax.optimization_barrier((weight, left_in))
    weight = exchange(weight, "col", LINES_OF_X)
    sketch, left_rows = call(
        sketch_kernel,
        [((ROWS * 18, 128), BF16), ((384, 384), BF16)],
        left_in, weight,
        scratch=[((ROWS * 10, 128), F32), ((384, 384), BF16), ((384, 384), BF16), ((ROWS * 18, 128), F32)],
    )
    sketch = exchange_lines(sketch, 18)
    own, sketch = call(
        total_kernel,
        [((24, 128), BF16), ((ROWS * 18, 128), BF16)],
        sketch,
        scratch=[((72, 128), F32), ((144, 128), F32)],
    )
    sketch = exchange_lines(sketch, 18)
    other = swap(sketch)
    (value,) = call(
        value_kernel,
        [((576, 128), BF16)],
        gate, sketch, left_rows,
        smem=1,
        scratch=[((ROWS * 18, 128), F32), ((384, 384), BF16), ((192, 384), F32)],
    )
    (value,) = call(
        gram_kernel,
        [((4, 984, 128), BF16)],
        place, sketch, other, value, own,
        smem=1,
        scratch=[((2, 128, 128), F32)],
    )
    value = exchange(value, "col", LINES_OF_X)
    (value,) = call(middle_kernel, [((1632, 128), BF16)], value)
    basis, block = call(
        last_kernel,
        [((72, 256), F32), ((ROWS, 8, 768), BF16)],
        place, value, swap(value), right,
        smem=1,
        scratch=[
            ((256, 256), F32), ((256, 256), F32), ((256, 256), F32), ((72, 256), F32),
            ((2, 3, 192, 256), BF16), ((256, 1536), F32),
        ],
    )
    block = exchange(block, "row")
    (new_block,) = call(block_kernel, [((4, 1536), F32)], block)
    return basis, new_block


def solution(mesh):
    return jax.shard_map(
        local,
        mesh=mesh,
        in_specs=(P("row", None, None), P("row", None, "col"), P(), P("col", None)),
        out_specs=(P("row", None), P("row", "col")),
        check_vma=False,
    )
```

```python
import jax
import jax.numpy as jnp
from jax import lax
from jax.experimental import pallas as pl
from jax.experimental.pallas import tpu as pltpu
from jax.sharding import PartitionSpec as P


F32 = jnp.float32
BF16 = jnp.bfloat16
HIGHEST = lax.Precision.HIGHEST
ROWS = 64
COLS = 8


def iota(shape, axis):
    return lax.broadcasted_iota(jnp.int32, shape, axis)


def dot(a, b, dims=((1,), (0,)), precision=None):
    return lax.dot_general(a, b, (dims, ((), ())), precision=precision, preferred_element_type=F32)


def stride_three(t, transposed):
    shape = (384, 128) if transposed else (128, 384)
    b, column = iota(shape, int(transposed)), iota(shape, int(not transposed))
    return jnp.where(column == 3 * b + t, 1.0, 0.0).astype(BF16)


def left_kernel(place, left, left_out, lines):
    row, column, lane = iota((16, 72), 0), iota((16, 72), 1), iota((16, 128), 1)
    sides = []
    for h in range(2):
        line = 2 * row + h
        photon = jnp.where(line < 6, 0, jnp.where(line < 12, 1, 2))
        chosen = (column == photon * 24 + 6 * (place[1] // 2) + line - 6 * photon) & (line < 18)
        sides.append(dot(jnp.where(chosen, 1.0, 0.0).astype(BF16), left[...].reshape(72, 4096)))
    for pair in range(ROWS // 2):
        even, odd = (side[:, 128 * pair : 128 * pair + 128] for side in sides)
        first = jnp.where(lane < 64, even, pltpu.roll(odd, 64, 1))
        second = jnp.where(lane < 64, pltpu.roll(even, 64, 1), odd)
        lines[20 * pair : 20 * pair + 10, :] = first[:10]
        lines[20 * pair + 10 : 20 * pair + 20, :] = second[:10]
    left_out[...] = lines[: ROWS * 10, :].astype(BF16)


def first_kernel(place, gate, right, probes, kept, sent, product):
    core = place[1] % 2
    wide = right[...].reshape(192, 512)
    for t in range(3):
        pick = stride_three(t, False)
        own = [dot(pick, probes[384 * j : 384 * j + 384, :]).astype(BF16) for j in range(4)]
        product[t] = dot(wide, jnp.concatenate(own, axis=0))
    for out, k in ((sent, 1 - core), (kept, core)):
        half = pl.ds(pl.multiple_of(128 * k, 128), 128)
        for up in range(3):
            for s in range(3):
                total = jnp.zeros((64, 128), F32)
                for tp in range(3):
                    for t in range(3):
                        total = total + gate[3 * s + t, 3 * up + tp] * product[t, 64 * tp : 64 * tp + 64, half]
                out[64 * up : 64 * up + 64, 128 * s : 128 * s + 128] = total


def weight_kernel(kept, received, out):
    total = (kept[...] + received[...]).astype(BF16)
    for x in range(4):
        out[x] = total


def sketch_kernel(left_in, weight, sketch_out, left_rows, wide_left, high, low, wide_sketch):
    wide_left[...] = left_in[...].astype(F32)
    side = iota((64, 128), 1) // 64
    for up in range(3):
        for i in range(6):
            line = 6 * up + i
            tile = jnp.where(side == line % 2, wide_left[pl.ds(line // 2, 64, stride=10), :], 0.0)
            left_rows[64 * i : 64 * i + 64, 128 * up : 128 * up + 128] = tile.astype(BF16)
    total = (weight[0].astype(F32) + weight[1].astype(F32)) + (weight[2].astype(F32) + weight[3].astype(F32))
    for part, wide in zip(split(total), (high, low)):
        for up in range(3):
            block = part[64 * up : 64 * up + 64]
            wide[128 * up : 128 * up + 64, :] = block
            wide[128 * up + 64 : 128 * up + 128, :] = block
    for i in range(6):
        rows = left_rows[64 * i : 64 * i + 64, :]
        part = dot(rows, high[...]) + dot(rows, low[...])
        for s in range(3):
            wide_sketch[pl.ds(3 * i + s, 64, stride=18), :] = part[:, 128 * s : 128 * s + 128]
    sketch_out[...] = wide_sketch[...].astype(BF16)


def total_kernel(pieces, own, out, four, many):
    total = pieces[:144, :].astype(F32)
    for k in range(1, 8):
        total = total + pieces[144 * k : 144 * k + 144, :].astype(F32)
    four[:72, :] = total[:72] + total[72:]
    total = four[0:18, :] + four[18:36, :] + four[36:54, :] + four[54:72, :]
    own[:18, :] = total.astype(BF16)
    own[18:, :] = jnp.zeros((6, 128), BF16)
    for k in range(8):
        many[18 * k : 18 * k + 18, :] = total
    total = many[:144, :].astype(BF16)
    for k in range(8):
        out[144 * k : 144 * k + 144, :] = total


def value_kernel(gate, sketch_in, left_rows, out, wide_sketch, sketch, product):
    wide_sketch[...] = sketch_in[...].astype(F32)
    for i in range(6):
        for s in range(3):
            tile = wide_sketch[pl.ds(3 * i + s, 64, stride=18), :]
            sketch[64 * i : 64 * i + 64, 128 * s : 128 * s + 128] = tile.astype(BF16)
    for up in range(3):
        part = dot(left_rows[:, 128 * up : 128 * up + 128], sketch[...], ((0,), (0,)))
        product[64 * up : 64 * up + 64, :] = part[:64] + part[64:]
    for tp in range(3):
        for t in range(3):
            total = jnp.zeros((64, 128), F32)
            for up in range(3):
                for s in range(3):
                    part = product[64 * up : 64 * up + 64, 128 * s : 128 * s + 128]
                    total = total + gate[3 * s + t, 3 * up + tp] * part
            line = 64 * (3 * tp + t)
            out[line : line + 64, :] = total.astype(BF16)


def gram_kernel(place, sketch_in, other_in, value, own, out, cross):
    core = place[1] % 2
    mine, other = sketch_in[...], other_in[...]
    block = dot(mine, mine, ((0,), (0,)))
    cross[0] = dot(other, mine, ((0,), (0,)))
    cross[1] = dot(mine, other, ((0,), (0,)))
    half = cross[core, pl.ds(pl.multiple_of(64 * core, 64), 64), :]
    block, half = split(block), split(half)
    for x in range(4):
        out[x, :576, :] = value[...]
        for part in range(2):
            out[x, 576 + 192 * part : 704 + 192 * part, :] = block[part]
            out[x, 704 + 192 * part : 768 + 192 * part, :] = half[part]
        out[x, 960:984, :] = own[...]


def middle_kernel(pieces, out):
    total = (pieces[0, :960].astype(F32) + pieces[1, :960].astype(F32)) + (
        pieces[2, :960].astype(F32) + pieces[3, :960].astype(F32)
    )
    value, gram = split(total[:576]), split(total[576:768] + total[768:960])
    out[:576, :] = value[0]
    out[576:1152, :] = value[1]
    out[1152:1344, :] = gram[0]
    out[1344:1536, :] = gram[1]
    for x in range(4):
        out[1536 + 24 * x : 1560 + 24 * x, :] = pieces[x, 960:984, :]


def split(value):
    high = value.astype(BF16)
    return high, (value - high.astype(F32)).astype(BF16)


def small_inverse(block):
    row, lane, sub = iota((64, 128), 0), iota((64, 128), 1), iota((8, 128), 0)
    diagonal = jnp.where(lane == row, block, 0.0)
    tall = lax.rsqrt(jnp.sum(diagonal, axis=1, keepdims=True))
    flat = jnp.sum(diagonal, axis=0, keepdims=True)
    flat = lax.rsqrt(jnp.where(iota((1, 128), 1) < 64, flat, 1.0))
    tail = jnp.where(lane < 64, block * tall * flat, jnp.where(lane - 64 == row, 1.0, 0.0)).reshape(8, 8, 128)
    done = []
    for k in range(0, 64, 8):
        head, tail = tail[0], tail[1:]
        count = tail.shape[0]
        lines = [jnp.broadcast_to(head[i : i + 1, :], (8, 128)) for i in range(8)]
        corner = [
            [jnp.broadcast_to(lines[i][:, k + j : k + j + 1], (8, 128)) if j >= i else None for j in range(8)]
            for i in range(8)
        ]
        if count:
            sides = [jnp.broadcast_to(tail[:, :, k + j : k + j + 1], tail.shape) for j in range(8)]
        for i in range(0, 8, 2):
            first, both, second = corner[i][i], corner[i][i + 1], corner[i + 1][i + 1]
            inverse = 1.0 / first
            ratio = both * inverse
            inverse_two = first * (1.0 / (first * second - both * both))
            lines[i + 1] = lines[i + 1] - ratio * lines[i]
            above, below = lines[i] * inverse, lines[i + 1] * inverse_two
            upper = corner[i]
            lower = [None if m <= i + 1 else corner[i + 1][m] - ratio * upper[m] for m in range(8)]
            if count:
                sides[i + 1] = sides[i + 1] - ratio * sides[i]
                tail = tail - (sides[i] * above + sides[i + 1] * below)
            for j in range(i + 2, 8):
                one, two = upper[j] * inverse, lower[j] * inverse_two
                lines[j] = lines[j] - (one * lines[i] + two * lines[i + 1])
                if count:
                    sides[j] = sides[j] - (one * sides[i] + two * sides[i + 1])
                for m in range(j, 8):
                    corner[j][m] = corner[j][m] - (one * upper[m] + two * lower[m])
        head = lines[7]
        for i in range(7):
            head = jnp.where(sub == i, lines[i], head)
        done.append(head)
    work = jnp.concatenate(done, axis=0)
    pivots = jnp.sum(jnp.where(lane == row, work, 0.0), axis=1, keepdims=True)
    return (work * lax.rsqrt(pivots))[:, 64:128] * flat[:, :64]


def last_kernel(place, mine, other, right, basis_out, block_out, gram, rest, inverse, sketch, value, result):
    core = place[1] % 2
    halves = [(side, pl.ds(pl.multiple_of(128 * k, 128), 128), k) for side, k in ((mine, core), (other, 1 - core))]
    for pieces, half, k in halves:
        whole = pieces[1152:1344, :].astype(F32) + pieces[1344:1536, :].astype(F32)
        gram[half, half] = whole[:128]
        gram[pl.ds(pl.multiple_of(128 + 64 * k, 64), 64), :128] = whole[128:]
    gram[:128, 128:] = gram[128:, :128].T
    rest[...] = jnp.where(iota((256, 256), 0) == iota((256, 256), 1), 1.0, 0.0)
    inverse[...] = jnp.zeros((256, 256), F32)
    for step in range(4):
        top, tile = 64 * step, 128 * (step // 2)
        ahead, behind = (tile if step % 2 == 0 else 128), tile + 128
        block = gram[top : top + 64, tile : tile + 128]
        small = small_inverse(pltpu.roll(block, 64, 1) if step % 2 else block)
        lines = rest[top : top + 64, :behind]
        if step < 3:
            lines = jnp.concatenate([gram[top : top + 64, ahead:], lines], axis=1)
        lines = dot(small, lines, precision=HIGHEST)
        inverse[top : top + 64, :behind] = lines[:, lines.shape[1] - behind :]
        if step < 3:
            below = dot(lines[:, : 256 - ahead], lines, ((0,), (0,)), precision=HIGHEST)[top + 64 - ahead :]
            gram[top + 64 :, ahead:] = gram[top + 64 :, ahead:] - below[:, : 256 - ahead]
            rest[top + 64 :, :behind] = rest[top + 64 :, :behind] - below[:, 256 - ahead :]
    for pieces, half, _ in halves:
        for x in range(4):
            rows = pieces[1536 + 24 * x : 1560 + 24 * x, :].astype(F32)
            sketch[18 * x : 18 * x + 18, half] = rows[:18]
    high, low = split(inverse[...])
    own = sketch[:72, :].astype(BF16)
    basis_out[...] = dot(own, high, ((1,), (1,))) + dot(own, low, ((1,), (1,)))
    for part in range(2):
        for pieces, half, _ in halves:
            for tp in range(3):
                for t in range(3):
                    line = 576 * part + 64 * (3 * tp + t)
                    value[part, t, 64 * tp : 64 * tp + 64, half] = pieces[line : line + 64, :]
    wide = right[...].reshape(192, 512)
    for t in range(3):
        mixed = dot(high, value[0, t], ((1,), (1,))) + dot(low, value[0, t], ((1,), (1,)))
        mixed = mixed + dot(high, value[1, t], ((1,), (1,)))
        first, second = split(mixed)
        result[:, 512 * t : 512 * t + 512] = dot(first, wide) + dot(second, wide)
    upper = iota((8, 768), 0) < 4
    for pair in range(ROWS // 2):
        first = result[8 * pair : 8 * pair + 8, :768]
        second = result[8 * pair : 8 * pair + 8, 768:]
        block_out[2 * pair] = jnp.where(upper, first, pltpu.roll(second, 4, 0)).astype(BF16)
        block_out[2 * pair + 1] = jnp.where(upper, pltpu.roll(first, 4, 0), second).astype(BF16)


def block_kernel(pieces, out):
    total = jnp.sum(pieces[...].astype(F32), axis=0)
    picks = [stride_three(t, False) for t in range(3)]
    for j in range(4):
        lines = jnp.zeros((4, 384), F32)
        for t in range(3):
            start = 512 * t + 128 * j
            half, start = start // 768, start % 768
            rest = total[:, start : start + 128]
            spread = jnp.zeros((8, 384), F32)
            for _ in range(3):
                part = rest.astype(BF16)
                spread = spread + dot(part, picks[t])
                rest = rest - part.astype(F32)
            lines = lines + spread[4 * half : 4 * half + 4]
        out[:, 384 * j : 384 * j + 384] = lines


SMEM = pl.BlockSpec(memory_space=pltpu.SMEM)
VMEM = pl.BlockSpec(memory_space=pltpu.VMEM)
INTERPRET = False


def call(kernel, out, *args, smem=0, scratch=()):
    return pl.pallas_call(
        kernel,
        out_shape=[jax.ShapeDtypeStruct(*o) for o in out],
        in_specs=[SMEM] * smem + [VMEM] * (len(args) - smem),
        out_specs=[VMEM] * len(out),
        scratch_shapes=[pltpu.VMEM(*s) for s in scratch],
        compiler_params=pltpu.CompilerParams(vmem_limit_bytes=48 * 1024 * 1024),
        interpret=INTERPRET,
    )(*args)


LINES_OF_X = [[0, 2, 4, 6], [1, 3, 5, 7]]


def exchange(value, axis, groups=None):
    return lax.all_to_all(value, axis, 0, 0, axis_index_groups=groups)


def exchange_lines(value, lines):
    return exchange(value.reshape(ROWS, lines // 2, 2, 128), "row").reshape(ROWS * lines, 128)


def swap(value):
    return lax.ppermute(value, "col", [(q, q ^ 1) for q in range(COLS)])


def local(left_site, right_site, gate, probes_matrix):
    place = jnp.stack([lax.axis_index("row"), lax.axis_index("col")]).astype(jnp.int32)
    left = left_site.transpose(1, 0, 2)
    right = right_site.transpose(1, 0, 2)
    (left_out,) = call(
        left_kernel, [((ROWS * 10, 128), BF16)], place, left, smem=1, scratch=[((ROWS * 10 + 8, 128), F32)]
    )
    left_in = exchange_lines(left_out, 10)
    kept, sent = call(
        first_kernel,
        [((192, 384), F32), ((192, 384), F32)],
        place, gate, right, probes_matrix,
        smem=2,
        scratch=[((3, 192, 256), F32)],
    )
    received = swap(sent)
    (weight,) = call(weight_kernel, [((4, 192, 384), BF16)], kept, received)
    weight, left_in = lax.optimization_barrier((weight, left_in))
    weight = exchange(weight, "col", LINES_OF_X)
    sketch, left_rows = call(
        sketch_kernel,
        [((ROWS * 18, 128), BF16), ((384, 384), BF16)],
        left_in, weight,
        scratch=[((ROWS * 10, 128), F32), ((384, 384), BF16), ((384, 384), BF16), ((ROWS * 18, 128), F32)],
    )
    sketch = exchange_lines(sketch, 18)
    own, sketch = call(
        total_kernel,
        [((24, 128), BF16), ((ROWS * 18, 128), BF16)],
        sketch,
        scratch=[((80, 128), F32), ((152, 128), F32)],
    )
    sketch = exchange_lines(sketch, 18)
    other = swap(sketch)
    (value,) = call(
        value_kernel,
        [((576, 128), BF16)],
        gate, sketch, left_rows,
        smem=1,
        scratch=[((ROWS * 18, 128), F32), ((384, 384), BF16), ((192, 384), F32)],
    )
    (value,) = call(
        gram_kernel,
        [((4, 984, 128), BF16)],
        place, sketch, other, value, own,
        smem=1,
        scratch=[((2, 128, 128), F32)],
    )
    value = exchange(value, "col", LINES_OF_X)
    (value,) = call(middle_kernel, [((1632, 128), BF16)], value)
    basis, block = call(
        last_kernel,
        [((72, 256), F32), ((ROWS, 8, 768), BF16)],
        place, value, swap(value), right,
        smem=1,
        scratch=[
            ((256, 256), F32), ((256, 256), F32), ((256, 256), F32), ((80, 256), F32),
            ((2, 3, 192, 256), BF16), ((256, 1536), F32),
        ],
    )
    block = exchange(block, "row")
    (new_block,) = call(block_kernel, [((4, 1536), F32)], block)
    return basis, new_block


def solution(mesh):
    return jax.shard_map(
        local,
        mesh=mesh,
        in_specs=(P("row", None, None), P("row", None, "col"), P(), P("col", None)),
        out_specs=(P("row", None), P("row", "col")),
        check_vma=False,
    )
```
